512 devices in a mesh: ra: 128 (over x_lo, y, z), dec: 4 (over x_hi, core).
Axes of the slice: x: 4 (x_hi: 2, x_lo: 2; x = x_hi * 2 + x_lo), y: 8, z: 8, core: 2. Of those that a mesh axis runs over, the one named last changes fastest.
Arguments:
- exposures: float32 [2, 1280, 49152], P(None, 'dec', 'ra'), may hold values from -6 to 6
- inv_variance: float32 [2, 1280, 49152], P(None, 'dec', 'ra'), may hold values from 0.25 to 4
- pixel_valid: int32 [2, 1280, 49152], P(None, 'dec', 'ra'), may hold values 0 or 1
- correlation: int32 [4, 128, 2], P('dec', 'ra'), may hold values 0 or 1
- pixel_offset: int32 [4, 128, 2, 2], P('dec', 'ra'), may hold values from -3 to 3
- subpixel: float32 [4, 128, 2, 2], P('dec', 'ra'), may hold values from -0.5 to 0.5
- psf_match: bfloat16 [63, 63], replicated, may hold values from -0.09375 to 0.09375
Outputs:
- matched: float32 [768, 32768], P('dec', 'ra')
- weight_map: float32 [768, 32768], P('dec', 'ra')
The draws below stay inside these ranges and needn't reach their ends.
All inputs are finite; a program needn't handle non-finite values. No bound on the sum of `pixel_valid` or of `correlation` on one device may be relied on, other than what follows from the above.
Results may differ from the reference program's by a relative error of at most 0.007.
Values may be sent and summed in bfloat16 or wider, within the bound.
No kernel may reach another device: no remote copies, remote signals or barrier semaphores. Data moves between devices by JAX's collectives and lax.ppermute only.
A program may use at most 128 MiB of HBM per device.

```python
import math
import jax
import jax.numpy as jnp
from jax import lax

MARGIN = 64
KERNEL = 63
EPOCHS = 2
HALF = 31
PROWS = 320
PCOLS = 384
STRIPS = 4
TILES = 128
NROWS = 768
NCOLS = 32768
SROWS = 1280
SCOLS = 49152


def with_ends(drawn, own_key, least, high):
    place = [jax.random.randint(jax.random.fold_in(own_key, axis), (), 0, length) for axis, length in enumerate(drawn.shape)]
    longest = drawn.shape.index(max(drawn.shape))
    neighbour = place[:longest] + [(place[longest] + 1) % drawn.shape[longest]] + place[longest + 1:]
    return drawn.at[tuple(place)].set(least).at[tuple(neighbour)].set(high)


def levels(rng, extent, pieces, low, high):
    loudness = 1.0
    for position, shards_of in pieces:
        steps = jax.random.uniform(jax.random.fold_in(jax.random.fold_in(rng, 6), position), (shards_of,), jnp.float32, low / len(pieces), high / len(pieces))
        loudness = loudness * jnp.repeat(jnp.exp(steps), extent[position] // shards_of).reshape((-1,) + (1,) * (len(extent) - 1 - position))
    return loudness


def centred(stream_key, extent, width, bound, shards=(), kind=jnp.bfloat16):
    values = width * jax.random.normal(stream_key, extent, jnp.float32)
    if shards:
        values = values * levels(stream_key, extent, shards, -0.22, 0.18)
    return jnp.clip(values, -bound, bound).astype(kind)


def setup_inputs(seed: int = 0) -> dict:
    arg_keys = jax.random.split(jax.random.key(seed), 8)
    return {
        "exposures": centred(arg_keys[0], (EPOCHS, SROWS, SCOLS), 1.0, 6.0, ((1, 4), (2, 128)), jnp.float32),
        "inv_variance": jnp.clip(jnp.exp(math.log(4.0) - 2.7725887 * jax.random.uniform(arg_keys[1], (EPOCHS, SROWS, SCOLS), jnp.float32) ** levels(arg_keys[1], (EPOCHS, SROWS, SCOLS), ((1, 4), (2, 128)), -0.2, 0.2)), 0.25, 4.0),
        "pixel_valid": with_ends((jax.random.randint(arg_keys[2], (EPOCHS, SROWS, SCOLS), 0, 8) < 7).astype(jnp.int32), jax.random.fold_in(arg_keys[2], 1), 0, 1),
        "correlation": with_ends((jax.random.randint(arg_keys[3], (STRIPS, TILES, EPOCHS), 0, 4) < 3).astype(jnp.int32), jax.random.fold_in(arg_keys[3], 1), 0, 1),
        "pixel_offset": with_ends(jax.random.randint(arg_keys[4], (STRIPS, TILES, EPOCHS, 2), -3, 4), jax.random.fold_in(arg_keys[4], 1), -3, 3).astype(jnp.int32),
        "subpixel": jnp.clip(jax.random.uniform(arg_keys[5], (STRIPS, TILES, EPOCHS, 2), jnp.float32, -0.5, 0.5) * levels(arg_keys[5], (STRIPS, TILES, EPOCHS, 2), ((0, 4), (1, 128)), -0.4, 0.0), -0.5, 0.5),
        "psf_match": centred(arg_keys[6], (KERNEL, KERNEL), (KERNEL * KERNEL) ** -0.5, 0.09375),
    }


HIGHEST_PRECISION = lax.Precision.HIGHEST


def lanczos_matrix(size_count, shift_value):
    row_ids = jnp.arange(size_count, dtype=jnp.int32)[:, None]
    col_ids = jnp.arange(size_count, dtype=jnp.int32)[None, :]
    where_at = (row_ids - col_ids).astype(shift_value.dtype) + shift_value
    kernel_value = jnp.sinc(where_at) * jnp.sinc(where_at / 3.0)
    return jnp.where(jnp.abs(where_at) < 3.0, kernel_value, jnp.zeros_like(kernel_value))


def warp_tile(images, weights, valid_bits, offsets, fractions, covered):
    row_count, col_count = images.shape[1], images.shape[2]
    numerator = jnp.zeros((row_count, col_count), images.dtype)
    denominator = jnp.zeros((row_count, col_count), images.dtype)
    for which_epoch in range(images.shape[0]):
        shifts = offsets[which_epoch].astype(fractions.dtype) + fractions[which_epoch]
        row_map = lanczos_matrix(row_count, shifts[0])
        col_map = lanczos_matrix(col_count, shifts[1])
        masked = weights[which_epoch] * valid_bits[which_epoch].astype(weights.dtype) * covered[which_epoch].astype(weights.dtype)
        stacked = jnp.concatenate([masked * images[which_epoch], masked], axis=1)
        half_done = jnp.dot(row_map, stacked, precision=HIGHEST_PRECISION)
        numerator = numerator + jnp.dot(half_done[:, :col_count], col_map.T, precision=HIGHEST_PRECISION)
        denominator = denominator + jnp.dot(half_done[:, col_count:], col_map.T, precision=HIGHEST_PRECISION)
    return numerator, denominator


def shift_tiles(values, grid_axis, offset_by, wrapping):
    if wrapping:
        return jnp.roll(values, offset_by, axis=grid_axis)
    size_count = values.shape[grid_axis]
    empty_slab = jnp.zeros_like(lax.slice_in_dim(values, 0, 1, axis=grid_axis))
    if offset_by > 0:
        return jnp.concatenate([empty_slab, lax.slice_in_dim(values, 0, size_count - 1, axis=grid_axis)], axis=grid_axis)
    return jnp.concatenate([lax.slice_in_dim(values, 1, size_count, axis=grid_axis), empty_slab], axis=grid_axis)


def place_margins(values, pixel_axis, grid_axis, wrapping):
    inner_size = values.shape[pixel_axis] - 2 * MARGIN
    summed = lax.slice_in_dim(values, MARGIN, MARGIN + inner_size, axis=pixel_axis)
    from_lower = shift_tiles(lax.slice_in_dim(values, MARGIN + inner_size, inner_size + 2 * MARGIN, axis=pixel_axis), grid_axis, 1, wrapping)
    from_upper = shift_tiles(lax.slice_in_dim(values, 0, MARGIN, axis=pixel_axis), grid_axis, -1, wrapping)
    pad_lower = [(0, 0)] * values.ndim
    pad_lower[pixel_axis] = (0, inner_size - MARGIN)
    pad_upper = [(0, 0)] * values.ndim
    pad_upper[pixel_axis] = (inner_size - MARGIN, 0)
    return summed + jnp.pad(from_lower, pad_lower) + jnp.pad(from_upper, pad_upper)


def reference(exposures, inv_variance, pixel_valid, correlation, pixel_offset, subpixel, psf_match):
    tile_count = STRIPS * TILES

    def one_tile(flat_index):
        strip_index = flat_index // TILES
        tile_index = flat_index - strip_index * TILES

        def tile_block(source):
            starts = (jnp.zeros((), jnp.int32), (strip_index * PROWS).astype(jnp.int32), (tile_index * PCOLS).astype(jnp.int32))
            return lax.dynamic_slice(source, starts, (EPOCHS, PROWS, PCOLS))

        return warp_tile(tile_block(exposures), tile_block(inv_variance), tile_block(pixel_valid), pixel_offset[strip_index, tile_index], subpixel[strip_index, tile_index], correlation[strip_index, tile_index])

    numerator, denominator = lax.map(one_tile, jnp.arange(tile_count, dtype=jnp.int32))
    planes = jnp.stack([numerator, denominator]).reshape(2, STRIPS, TILES, PROWS, PCOLS)
    planes = place_margins(planes, 4, 2, True)
    planes = place_margins(planes, 3, 1, False)
    planes = planes.transpose(0, 1, 3, 2, 4).reshape(2, NROWS, NCOLS)
    weight_map = planes[1]
    coadded = (planes[0] / jnp.maximum(planes[1], 1.0)).astype(jnp.bfloat16)
    wrapped = jnp.concatenate([coadded[:, NCOLS - HALF:], coadded, coadded[:, :HALF]], axis=1)
    padded = jnp.pad(wrapped, ((HALF, HALF), (0, 0)))
    matched = lax.conv_general_dilated(padded.astype(jnp.float32)[None, None], psf_match.astype(jnp.float32)[None, None], (1, 1), "VALID", precision=HIGHEST_PRECISION)[0, 0]
    return matched, weight_map
```

```python
import jax
import jax.numpy as jnp
from jax import lax
from jax.experimental import pallas as pl
from jax.experimental.pallas import tpu as pltpu
from jax.sharding import PartitionSpec as P


ROWS = 192
COLS = 256
PROWS = 320
PCOLS = 384
BAND = 96
EXT = 256
HALF = 31
SIDE = 63
LEFT = 64 - HALF
TILES_K = 33
PI = 3.141592653589793
F32 = jnp.float32
BF16 = jnp.bfloat16


def swap_pairs(block, axis, start, wrap):
    count = lax.axis_size(axis)
    lows = [i for i in range(start, count, 2) if wrap or i + 1 < count]
    pairs = [(i, (i + 1) % count) for i in lows]
    return lax.ppermute(block, axis, pairs + [(b, a) for a, b in pairs])


def is_odd(axis):
    return (lax.axis_index(axis) & 1) == 1


def sin_pi(z):
    y = z * PI
    y2 = y * y
    poly = 1.0 / 6227020800.0
    for factorial in (-39916800.0, 362880.0, -5040.0, 120.0, -6.0, 1.0):
        poly = poly * y2 + 1.0 / factorial
    return y * poly


def lanczos_map(offset, fraction, direction):
    lane = lax.broadcasted_iota(jnp.int32, (8, 128), 1)
    signed = jnp.where(lane < 64, lane, lane - 128) * direction
    step = signed + offset
    where_at = step.astype(F32) + fraction
    parity = 1.0 - 2.0 * (step & 1).astype(F32)
    frac = jnp.full((8, 128), fraction, F32)
    third = jnp.abs(where_at) * (1.0 / 3.0)
    folded = jnp.where(third > 0.5, 1.0 - third, third)
    safe = jnp.where(where_at == 0.0, 1.0, where_at)
    first = parity * sin_pi(frac) / (safe * PI)
    second = sin_pi(folded) * 3.0 / (jnp.abs(safe) * PI)
    value = jnp.where(where_at == 0.0, 1.0, first * second)
    value = jnp.where(jnp.abs(where_at) < 3.0, value, 0.0)
    rows = jnp.broadcast_to(value[0:1], (128, 128))
    turned = pltpu.roll(rows, 0, 1, stride=1, stride_axis=0)
    down = lax.broadcasted_iota(jnp.int32, (128, 128), 0)
    across = lax.broadcasted_iota(jnp.int32, (128, 128), 1)
    gap = across - down
    diagonal = jnp.where(jnp.abs(gap) <= 64, turned, 0.0)
    upper = jnp.where(gap < -64, turned, 0.0)
    lower = jnp.where(gap > 64, turned, 0.0)
    return jnp.concatenate(
        [
            jnp.concatenate([diagonal, upper], axis=1),
            jnp.concatenate([lower, diagonal], axis=1),
        ],
        axis=0,
    )


def split(value):
    high = value.astype(BF16)
    return high, (value - high.astype(F32)).astype(BF16)


def dot(a, b):
    return lax.dot_general(a, b, (((1,), (0,)), ((), ())), preferred_element_type=F32)


def warp_kernel(
    off_hbm, sub_hbm, cov_hbm, exp_hbm, inv_hbm, val_hbm,
    own, near, far,
    off, sub, cov, exp, inv, val, small, large,
):
    scalars = [
        pltpu.make_async_copy(source, target, small.at[i])
        for i, (source, target) in enumerate(((off_hbm, off), (sub_hbm, sub), (cov_hbm, cov)))
    ]
    images = [
        [
            pltpu.make_async_copy(source.at[e], target.at[e], large.at[e, i])
            for i, (source, target) in enumerate(((inv_hbm, inv), (val_hbm, val), (exp_hbm, exp)))
        ]
        for e in range(2)
    ]
    for copy in scalars + images[0] + images[1]:
        copy.start()
    for copy in scalars:
        copy.wait()
    maps = [
        [
            split(lanczos_map(off[0, 0, e, axis], sub[0, 0, e, axis], direction))
            for axis, direction in ((0, -1), (1, 1))
        ]
        for e in range(2)
    ]
    first = [[None, None], [None, None]]
    for e in range(2):
        (row_high, row_low), (col_high, col_low) = maps[e]
        for copy in images[e]:
            copy.wait()
        covered = cov[0, 0, e].astype(F32)
        masked = inv[e] * (val[e].astype(F32) * covered)
        planes = (masked * exp[e], masked)
        for n in range(2):
            data = planes[n].astype(BF16)
            half_a = dot(row_high[:160], data[:256]) + dot(row_low[:160], data[:256])
            half_b = dot(row_high[96:], data[64:]) + dot(row_low[96:], data[64:])
            half = jnp.concatenate([half_a, half_b], axis=0).astype(BF16)
            for h in range(2):
                piece = half[:, 128 * h : 128 * h + 256]
                out = dot(piece, col_high) + dot(piece, col_low)
                first[n][h] = out if e == 0 else first[n][h] + out
    lane = lax.broadcasted_iota(jnp.int32, (PROWS, 128), 1)
    odd = is_odd("dec")
    for n in range(2):
        left, right = first[n]
        middle = jnp.where(lane < 64, left[:, 128:], right[:, :128])
        whole = jnp.concatenate([left[:, :128], middle, right[:, 128:]], axis=1)
        own[n] = whole[32 : 32 + EXT]
        top, bottom = whole[:BAND], whole[PROWS - BAND :]
        near[n] = jnp.where(odd, top, bottom).astype(BF16)
        far[n] = jnp.where(odd, bottom, top).astype(BF16)


def dec_sum(own, near, far, odd, n, block):
    cut = pl.ds(128 * block, 128)
    first, second = near[n, :, cut].astype(F32), far[n, :, cut].astype(F32)
    above, below = jnp.where(odd, first, second), jnp.where(odd, second, first)
    return [own[n, 0:96, cut] + above, own[n, 96:160, cut], own[n, 160:256, cut] + below]


def pack(planes):
    lane = lax.broadcasted_iota(jnp.int32, (128, 128), 1)
    groups = [plane[128 * i : 128 * i + 128] for plane in planes for i in range(2)]
    return jnp.concatenate(
        [
            jnp.where(lane < 96, groups[i], pltpu.roll(groups[3], 96 - 32 * i, 1))
            for i in range(3)
        ],
        axis=0,
    )


def unpack(packed):
    lane = lax.broadcasted_iota(jnp.int32, (128, 128), 1)
    groups = [packed[128 * i : 128 * i + 128] for i in range(3)]
    last = pltpu.roll(groups[0], 32, 1)
    last = jnp.where(lane < 32, last, pltpu.roll(groups[1], 64, 1))
    last = jnp.where(lane < 64, last, pltpu.roll(groups[2], 96, 1))
    groups.append(last)
    return [jnp.concatenate(groups[2 * n : 2 * n + 2], axis=0) for n in range(2)]


def edges_kernel(own, near, far, one, two):
    odd = is_odd("dec")
    west = pack([jnp.concatenate(dec_sum(own, near, far, odd, n, 0), axis=0) for n in range(2)])
    east = pack(
        [
            pltpu.roll(jnp.concatenate(dec_sum(own, near, far, odd, n, 2), axis=0), 96, 1)
            for n in range(2)
        ]
    )
    odd = is_odd("ra")
    one[...] = jnp.where(odd, west, east).astype(BF16)
    two[...] = jnp.where(odd, east, west).astype(BF16)


def psf_kernel(psf, weights, taps):
    down = lax.broadcasted_iota(jnp.int32, (SIDE, 128), 0)
    across = lax.broadcasted_iota(jnp.int32, (SIDE, 128), 1)
    reverse = jnp.where(((down + across) & 127) == 0, 1.0, 0.0).astype(BF16)
    taps[...] = jnp.zeros((80, 128), F32)
    taps[8 : 8 + SIDE] = dot(psf[...], reverse)
    lane = lax.broadcasted_iota(jnp.int32, (128, 128), 1)
    weights[0] = jnp.zeros((256, 128), BF16)
    weights[TILES_K] = jnp.zeros((256, 128), BF16)
    for q in range(64):
        here = jnp.broadcast_to(taps[8 + q : 9 + q], (128, 128))
        prev = jnp.broadcast_to(taps[7 + q : 8 + q], (128, 128))
        here = pltpu.roll(here, 0, 1, stride=1, stride_axis=0)
        prev = pltpu.roll(prev, 64, 1, stride=1, stride_axis=0)
        weights[1 + q // 2, 128 * (q % 2) : 128 * (q % 2) + 128] = jnp.where(
            lane < 64, here, prev
        ).astype(BF16)


def match_kernel(own, near, far, one, two, weights, out, weight_map, windows, stage):
    odd = is_odd("ra")
    first, second = one[...].astype(F32), two[...].astype(F32)
    west = [pltpu.roll(plane, 32, 1) for plane in unpack(jnp.where(odd, first, second))]
    east = unpack(jnp.where(odd, second, first))
    lane = lax.broadcasted_iota(jnp.int32, (EXT, 128), 1)
    odd = is_odd("dec")
    numer, denom = [], []
    for n, plane in ((0, numer), (1, denom)):
        for block in range(3):
            whole = jnp.concatenate(dec_sum(own, near, far, odd, n, block), axis=0)
            if block == 0:
                whole = whole + jnp.where(lane >= 32, west[n], 0.0)
            if block == 2:
                whole = whole + jnp.where(lane < 96, east[n], 0.0)
            plane.append(whole)
    denom = jnp.concatenate(denom, axis=1)
    numer = jnp.concatenate(numer, axis=1)
    row = lax.broadcasted_iota(jnp.int32, (EXT, PCOLS), 0) + (lax.axis_index("dec") * ROWS - 32)
    inside = (row >= 0) & (row < lax.axis_size("dec") * ROWS)
    coadd = jnp.where(inside, numer / jnp.maximum(denom, 1.0), 0.0).astype(BF16).astype(F32)
    weight_map[...] = pltpu.roll(denom, PCOLS - 64, 1)[32 : 32 + ROWS, :COLS]
    even = pltpu.roll(coadd, PCOLS - LEFT, 1)
    odd = pltpu.roll(coadd, PCOLS - LEFT - 64, 1)
    for k in range(4):
        source = odd if k % 2 else even
        windows[k, 0:EXT] = source[:, 128 * (k // 2) : 128 * (k // 2) + 128]
    total = None
    for t in range(TILES_K):
        left = jnp.concatenate(
            [
                jnp.concatenate(
                    [windows[k, pl.ds(2 * t + s + 1, 48, stride=4), :] for k in range(4)], axis=0
                )
                for s in range(2)
            ],
            axis=1,
        ).astype(BF16)
        right = jnp.concatenate([weights[t + 1], weights[t]], axis=1)
        part = dot(left, right)
        total = part if total is None else total + part
    lane = lax.broadcasted_iota(jnp.int32, (48, 128), 1)
    for h in range(2):
        lows = total[96 * h : 96 * h + 48]
        highs = total[96 * h + 48 : 96 * h + 96]
        for p in range(4):
            cut = slice(128 * (p // 2), 128 * (p // 2) + 128)
            low, high = lows[:, cut], highs[:, cut]
            if p % 2:
                low = pltpu.roll(low, 64, 1)
            else:
                high = pltpu.roll(high, 64, 1)
            stage[h, pl.ds(p, 48, stride=4), :] = jnp.where(lane < 64, low, high)
        out[:, 128 * h : 128 * h + 128] = stage[h]


HBM = pl.BlockSpec(memory_space=pltpu.HBM)
VMEM = pl.BlockSpec(memory_space=pltpu.VMEM)


def call(body, ins, outs, scratch=(), flops=0, limit=16):
    return pl.pallas_call(
        body,
        in_specs=ins,
        out_specs=tuple(VMEM for _ in outs),
        out_shape=outs,
        scratch_shapes=scratch,
        cost_estimate=pl.CostEstimate(flops=flops, transcendentals=0, bytes_accessed=4_000_000),
        compiler_params=pltpu.CompilerParams(vmem_limit_bytes=limit * 1024 * 1024),
    )


def array(shape, kind):
    return jax.ShapeDtypeStruct(shape, kind)


def shards(exposures, inv_variance, pixel_valid, correlation, pixel_offset, subpixel, psf_match):
    own, near, far = call(
        warp_kernel,
        [HBM] * 6,
        (array((2, EXT, PCOLS), F32), array((2, BAND, PCOLS), BF16), array((2, BAND, PCOLS), BF16)),
        scratch=[
            pltpu.SMEM((1, 1, 2, 2), jnp.int32),
            pltpu.SMEM((1, 1, 2, 2), F32),
            pltpu.SMEM((1, 1, 2), jnp.int32),
            pltpu.VMEM((2, PROWS, PCOLS), F32),
            pltpu.VMEM((2, PROWS, PCOLS), F32),
            pltpu.VMEM((2, PROWS, PCOLS), jnp.int32),
            pltpu.SemaphoreType.DMA((3,)),
            pltpu.SemaphoreType.DMA((2, 3)),
        ],
        flops=3_000_000_000,
    )(
        *(
            pltpu.with_memory_space_constraint(x, pltpu.HBM)
            for x in (pixel_offset, subpixel, correlation, exposures, inv_variance, pixel_valid)
        )
    )
    far = swap_pairs(far, "dec", 1, False)
    near = swap_pairs(near, "dec", 0, False)
    (weights,) = call(
        psf_kernel,
        [VMEM],
        (array((TILES_K + 1, 256, 128), BF16),),
        scratch=[pltpu.VMEM((80, 128), F32)],
        flops=3_000_000_000,
    )(psf_match)
    one, two = call(
        edges_kernel,
        [VMEM] * 3,
        (array((384, 128), BF16), array((384, 128), BF16)),
        flops=1_000_000,
    )(own, near, far)
    one = swap_pairs(one, "ra", 0, True)
    two = swap_pairs(two, "ra", 1, True)
    return call(
        match_kernel,
        [VMEM] * 6,
        (array((ROWS, COLS), F32), array((ROWS, COLS), F32)),
        scratch=[pltpu.VMEM((4, EXT + 8, 128), F32), pltpu.VMEM((2, ROWS, 128), F32)],
        flops=3_000_000_000,
    )(own, near, far, one, two, weights)


def solution(mesh):
    return jax.shard_map(
        shards,
        mesh=mesh,
        in_specs=(
            P(None, "dec", "ra"),
            P(None, "dec", "ra"),
            P(None, "dec", "ra"),
            P("dec", "ra", None),
            P("dec", "ra", None, None),
            P("dec", "ra", None, None),
            P(),
        ),
        out_specs=(P("dec", "ra"), P("dec", "ra")),
        check_vma=False,
    )
```

```python
import jax
import jax.numpy as jnp
from jax import lax
from jax.experimental import pallas as pl
from jax.experimental.pallas import tpu as pltpu
from jax.sharding import PartitionSpec as P


ROWS = 192
COLS = 256
PROWS = 320
PCOLS = 384
BAND = 96
EXT = 256
HALF = 31
SIDE = 63
LEFT = 64 - HALF
TILES_K = 33
PI = 3.141592653589793
F32 = jnp.float32
BF16 = jnp.bfloat16


def swap_pairs(block, axis, firsts, wrap):
    count = lax.axis_size(axis)
    lows = [i for i in range(count) if firsts(i) and (wrap or i + 1 < count)]
    if not lows:
        return jnp.zeros_like(block)
    pairs = [(i, (i + 1) % count) for i in lows]
    return lax.ppermute(block, axis, pairs + [(b, a) for a, b in pairs])


def is_odd(axis):
    return (lax.axis_index(axis) & 1) == 1


def sin_pi(z):
    y = z * PI
    y2 = y * y
    poly = 1.0 / 6227020800.0
    for factorial in (-39916800.0, 362880.0, -5040.0, 120.0, -6.0, 1.0):
        poly = poly * y2 + 1.0 / factorial
    return y * poly


def lanczos_map(offset, fraction, direction):
    lane = lax.broadcasted_iota(jnp.int32, (8, 128), 1)
    signed = jnp.where(lane < 64, lane, lane - 128) * direction
    step = signed + offset
    where_at = step.astype(F32) + fraction
    parity = 1.0 - 2.0 * (step & 1).astype(F32)
    frac = jnp.full((8, 128), fraction, F32)
    third = jnp.abs(where_at) * (1.0 / 3.0)
    folded = jnp.where(third > 0.5, 1.0 - third, third)
    safe = jnp.where(where_at == 0.0, 1.0, where_at)
    first = parity * sin_pi(frac) / (safe * PI)
    second = sin_pi(folded) * 3.0 / (jnp.abs(safe) * PI)
    value = jnp.where(where_at == 0.0, 1.0, first * second)
    value = jnp.where(jnp.abs(where_at) < 3.0, value, 0.0)
    rows = jnp.broadcast_to(value[0:1], (128, 128))
    turned = pltpu.roll(rows, 0, 1, stride=1, stride_axis=0)
    down = lax.broadcasted_iota(jnp.int32, (128, 128), 0)
    across = lax.broadcasted_iota(jnp.int32, (128, 128), 1)
    gap = across - down
    diagonal = jnp.where(jnp.abs(gap) <= 64, turned, 0.0)
    upper = jnp.where(gap < -64, turned, 0.0)
    lower = jnp.where(gap > 64, turned, 0.0)
    return diagonal, upper, lower


def row_map(offset, fraction):
    return jnp.concatenate(split(lanczos_map(offset, fraction, -1)[0]), axis=1)


def col_map(offset, fraction):
    diagonal, upper, lower = lanczos_map(offset, fraction, 1)
    return split(
        jnp.concatenate(
            [
                jnp.concatenate([diagonal, upper], axis=1),
                jnp.concatenate([lower, diagonal], axis=1),
            ],
            axis=0,
        )
    )


def split(value):
    high = value.astype(BF16)
    return high, (value - high.astype(F32)).astype(BF16)


def dot(a, b):
    return lax.dot_general(a, b, (((1,), (0,)), ((), ())), preferred_element_type=F32)


def joined(left, right):
    lane = lax.broadcasted_iota(jnp.int32, left[:, :128].shape, 1)
    middle = jnp.where(lane < 64, left[:, 128:], right[:, :128])
    return jnp.concatenate([left[:, :128], middle, right[:, 128:]], axis=1)


def warp_cols(halves, cols):
    planes = []
    for n in range(2):
        sides = []
        for h in range(2):
            at = PCOLS * n + 128 * h
            parts = [
                dot(half[:, at : at + 256], part)
                for half, pair in zip(halves, cols)
                for part in pair
            ]
            sides.append((parts[0] + parts[1]) + (parts[2] + parts[3]))
        planes.append(joined(*sides))
    return planes


def warp_kernel(
    off_hbm, sub_hbm, cov_hbm, exp_hbm, inv_hbm, val_hbm,
    own, near, far, middle, row_maps, col_maps,
    off, sub, cov, exp, inv, val, small, large,
):
    scalars = [
        pltpu.make_async_copy(source, target, small.at[i])
        for i, (source, target) in enumerate(((off_hbm, off), (sub_hbm, sub), (cov_hbm, cov)))
    ]
    images = [
        [
            pltpu.make_async_copy(source.at[e], target.at[e], large.at[e, i])
            for i, (source, target) in enumerate(((inv_hbm, inv), (val_hbm, val), (exp_hbm, exp)))
        ]
        for e in range(2)
    ]
    for copy in scalars + images[0] + images[1]:
        copy.start()
    for copy in scalars:
        copy.wait()
    rows = [row_map(off[0, 0, e, 0], sub[0, 0, e, 0]) for e in range(2)]
    cols = [col_map(off[0, 0, e, 1], sub[0, 0, e, 1]) for e in range(2)]
    halves = []
    for e in range(2):
        row_maps[e] = rows[e]
        col_maps[e, 0], col_maps[e, 1] = cols[e]
        for copy in images[e]:
            copy.wait()
        covered = cov[0, 0, e].astype(F32)
        masked = inv[e] * (val[e].astype(F32) * covered)
        data = jnp.concatenate([masked * exp[e], masked], axis=1).astype(BF16)
        middle[e] = data[96:224]
        halves.append(
            jnp.concatenate(
                [
                    dot(rows[e][low:high], jnp.concatenate([data[at : at + 128]] * 2, axis=0))
                    for at, low, high in ((0, 0, 112), (192, 16, 128))
                ],
                axis=0,
            ).astype(BF16)
        )
    odd = is_odd("dec")
    for n, whole in enumerate(warp_cols(halves, cols)):
        own[n, :80], own[n, 80:] = whole[32:112], whole[112:192]
        top, bottom = whole[:BAND], whole[128:]
        near[n] = jnp.where(odd, top, bottom).astype(BF16)
        far[n] = jnp.where(odd, bottom, top).astype(BF16)


def middle_kernel(middle, row_maps, col_maps, own):
    halves = [
        dot(row_maps[e, 16:112], jnp.concatenate([middle[e]] * 2, axis=0)).astype(BF16)
        for e in range(2)
    ]
    own[0], own[1] = warp_cols(halves, [(col_maps[e, 0], col_maps[e, 1]) for e in range(2)])


def dec_sum(own, mid, near, far, odd, n, block):
    cut = pl.ds(block * 128 if isinstance(block, int) else pl.multiple_of(block * 128, 128), 128)
    first, second = near[n, :, cut].astype(F32), far[n, :, cut].astype(F32)
    above, below = jnp.where(odd, first, second), jnp.where(odd, second, first)
    return jnp.concatenate(
        [
            own[n, :80, cut] + above[:80],
            mid[n, :16, cut] + above[80:],
            mid[n, 16:80, cut],
            mid[n, 80:, cut] + below[:16],
            own[n, 80:, cut] + below[16:],
        ],
        axis=0,
    )


def pack(planes):
    lane = lax.broadcasted_iota(jnp.int32, (128, 128), 1)
    groups = [plane[128 * i : 128 * i + 128] for plane in planes for i in range(2)]
    return jnp.concatenate(
        [
            jnp.where(lane < 96, groups[i], pltpu.roll(groups[3], 96 - 32 * i, 1))
            for i in range(3)
        ],
        axis=0,
    )


def unpack(packed):
    lane = lax.broadcasted_iota(jnp.int32, (128, 128), 1)
    groups = [packed[128 * i : 128 * i + 128] for i in range(3)]
    last = pltpu.roll(groups[0], 32, 1)
    last = jnp.where(lane < 32, last, pltpu.roll(groups[1], 64, 1))
    last = jnp.where(lane < 64, last, pltpu.roll(groups[2], 96, 1))
    groups.append(last)
    return [jnp.concatenate(groups[2 * n : 2 * n + 2], axis=0) for n in range(2)]


def edges_kernel(own, mid, near, far, one, two):
    odd = is_odd("dec")
    west = pack([dec_sum(own, mid, near, far, odd, n, 0) for n in range(2)])
    east = pack([pltpu.roll(dec_sum(own, mid, near, far, odd, n, 2), 96, 1) for n in range(2)])
    odd = is_odd("ra")
    one[...] = jnp.where(odd, west, east).astype(BF16)
    two[...] = jnp.where(odd, east, west).astype(BF16)


def psf_kernel(psf, weights, taps):
    down = lax.broadcasted_iota(jnp.int32, (SIDE, 128), 0)
    across = lax.broadcasted_iota(jnp.int32, (SIDE, 128), 1)
    reverse = jnp.where(((down + across) & 127) == 0, 1.0, 0.0).astype(BF16)
    taps[...] = jnp.zeros((80, 128), F32)
    taps[8 : 8 + SIDE] = dot(psf[...], reverse)
    lane = lax.broadcasted_iota(jnp.int32, (128, 128), 1)
    weights[0] = jnp.zeros((256, 128), BF16)
    weights[TILES_K] = jnp.zeros((256, 128), BF16)
    before = jnp.zeros((128, 128), F32)
    for q in range(64):
        here = jnp.broadcast_to(taps[8 + q : 9 + q], (128, 128))
        here = pltpu.roll(here, 0, 1, stride=1, stride_axis=0)
        prev = jnp.concatenate([before[64:], before[:64]], axis=0)
        weights[1 + q // 2, 128 * (q % 2) : 128 * (q % 2) + 128] = jnp.where(
            lane < 64, here, prev
        ).astype(BF16)
        before = here


def half_match(half, own, mid, near, far, bands, weights, weight, windows, stage):
    lane = lax.broadcasted_iota(jnp.int32, (EXT, 128), 1)
    east = half == 1
    odd = is_odd("dec")
    planes = []
    for n in range(2):
        band = unpack(bands)[n]
        band = jnp.where(
            east, jnp.where(lane < 96, band, 0.0), jnp.where(lane >= 32, pltpu.roll(band, 32, 1), 0.0)
        )
        left = dec_sum(own, mid, near, far, odd, n, half)
        right = dec_sum(own, mid, near, far, odd, n, half + 1)
        planes.append(
            jnp.concatenate(
                [left + jnp.where(east, 0.0, band), right + jnp.where(east, band, 0.0)], axis=1
            )
        )
    numer, denom = planes
    row = lax.broadcasted_iota(jnp.int32, (EXT, 256), 0) + (lax.axis_index("dec") * ROWS - 32)
    inside = (row >= 0) & (row < lax.axis_size("dec") * ROWS)
    coadd = jnp.where(inside, numer / jnp.maximum(denom, 1.0), 0.0).astype(BF16).astype(F32)
    weight(pltpu.roll(denom, 256 - 64, 1)[32 : 32 + ROWS, :128])
    for k in range(2):
        windows[k] = pltpu.roll(coadd, 256 - LEFT - 64 * k, 1)[:, :128]
    total = None
    for t in range(TILES_K):
        left = jnp.concatenate(
            [
                jnp.concatenate(
                    [windows[k, pl.ds(2 * t + s + 1, 48, stride=4), :] for k in range(2)], axis=0
                )
                for s in range(2)
            ],
            axis=1,
        ).astype(BF16)
        right = jnp.concatenate([weights[t + 1], weights[t]], axis=1)
        part = dot(left, right)
        total = part if total is None else total + part
    lane = lax.broadcasted_iota(jnp.int32, (48, 128), 1)
    for p in range(4):
        cut = slice(128 * (p // 2), 128 * (p // 2) + 128)
        low, high = total[:48, cut], total[48:, cut]
        if p % 2:
            low = pltpu.roll(low, 64, 1)
        else:
            high = pltpu.roll(high, 64, 1)
        stage[pl.ds(p, 48, stride=4), :] = jnp.where(lane < 64, low, high)


def first_kernel(own, mid, near, far, one, other, weights, out, weight_map, windows):
    def weight(value):
        weight_map[...] = value

    half = 1 - (lax.axis_index("ra") & 1)
    bands = one[...].astype(F32) + other[...].astype(F32)
    half_match(half, own, mid, near, far, bands, weights, weight, windows, out)


def second_kernel(
    own, mid, near, far, two, weights, ready, ready_weight,
    out, weight_map,
    windows, stage, stage_weight, sems,
):
    half = lax.axis_index("ra") & 1
    this, that = (pl.ds(pl.multiple_of(128 * x, 128), 128) for x in (half, 1 - half))
    copies = [
        pltpu.make_async_copy(source, target, sems.at[i])
        for i, (source, target) in enumerate(
            (
                (ready, out.at[:, that]),
                (ready_weight, weight_map.at[:, that]),
                (stage_weight, weight_map.at[:, this]),
                (stage, out.at[:, this]),
            )
        )
    ]
    copies[0].start()
    copies[1].start()

    def weight(value):
        stage_weight[...] = value
        copies[2].start()

    half_match(half, own, mid, near, far, two[...].astype(F32), weights, weight, windows, stage)
    copies[3].start()
    for copy in copies:
        copy.wait()


HBM = pl.BlockSpec(memory_space=pltpu.HBM)
VMEM = pl.BlockSpec(memory_space=pltpu.VMEM)


def call(body, ins, outs, scratch=(), flops=0, limit=16, space=None):
    return pl.pallas_call(
        body,
        in_specs=ins,
        out_specs=tuple(space or VMEM for _ in outs),
        out_shape=outs,
        scratch_shapes=scratch,
        cost_estimate=pl.CostEstimate(flops=flops, transcendentals=0, bytes_accessed=4_000_000),
        compiler_params=pltpu.CompilerParams(vmem_limit_bytes=limit * 1024 * 1024),
    )


def array(shape, kind):
    return jax.ShapeDtypeStruct(shape, kind)


def shards(exposures, inv_variance, pixel_valid, correlation, pixel_offset, subpixel, psf_match):
    own, near, far, middle, row_maps, col_maps = call(
        warp_kernel,
        [HBM] * 6,
        (
            array((2, 160, PCOLS), F32),
            array((2, BAND, PCOLS), BF16),
            array((2, BAND, PCOLS), BF16),
            array((2, 128, 2 * PCOLS), BF16),
            array((2, 128, 256), BF16),
            array((2, 2, 256, 256), BF16),
        ),
        scratch=[
            pltpu.SMEM((1, 1, 2, 2), jnp.int32),
            pltpu.SMEM((1, 1, 2, 2), F32),
            pltpu.SMEM((1, 1, 2), jnp.int32),
            pltpu.VMEM((2, PROWS, PCOLS), F32),
            pltpu.VMEM((2, PROWS, PCOLS), F32),
            pltpu.VMEM((2, PROWS, PCOLS), jnp.int32),
            pltpu.SemaphoreType.DMA((3,)),
            pltpu.SemaphoreType.DMA((2, 3)),
        ],
        flops=3_000_000_000,
    )(
        *(
            pltpu.with_memory_space_constraint(x, pltpu.HBM)
            for x in (pixel_offset, subpixel, correlation, exposures, inv_variance, pixel_valid)
        )
    )
    far = swap_pairs(far, "dec", lambda i: i % 2 == 1, False)
    near = swap_pairs(near, "dec", lambda i: i % 2 == 0, False)
    (weights,) = call(
        psf_kernel,
        [VMEM],
        (array((TILES_K + 1, 256, 128), BF16),),
        scratch=[pltpu.VMEM((80, 128), F32)],
        flops=3_000_000_000,
    )(psf_match)
    (mid,) = call(
        middle_kernel, [VMEM] * 3, (array((2, 96, PCOLS), F32),), flops=3_000_000_000
    )(middle, row_maps, col_maps)
    one, two = call(
        edges_kernel,
        [VMEM] * 4,
        (array((384, 128), BF16), array((384, 128), BF16)),
        flops=1_000_000,
    )(own, mid, near, far)
    first = swap_pairs(one, "ra", lambda i: i % 8 in (0, 2, 4), True)
    two = swap_pairs(two, "ra", lambda i: i % 2 == 1, True)
    last = swap_pairs(one, "ra", lambda i: i % 8 == 6, True)
    windows = pltpu.VMEM((2, EXT, 128), F32)
    stage = pltpu.VMEM((ROWS, 128), F32)
    ready, ready_weight = call(
        first_kernel,
        [VMEM] * 7,
        (array((ROWS, 128), F32), array((ROWS, 128), F32)),
        scratch=[windows],
        flops=3_000_000_000,
    )(own, mid, near, far, first, last, weights)
    return call(
        second_kernel,
        [VMEM] * 8,
        (array((ROWS, COLS), F32), array((ROWS, COLS), F32)),
        scratch=[windows, stage, stage, pltpu.SemaphoreType.DMA((4,))],
        flops=3_000_000_000,
        space=HBM,
    )(own, mid, near, far, two, weights, ready, ready_weight)


def solution(mesh):
    return jax.shard_map(
        shards,
        mesh=mesh,
        in_specs=(
            P(None, "dec", "ra"),
            P(None, "dec", "ra"),
            P(None, "dec", "ra"),
            P("dec", "ra", None),
            P("dec", "ra", None, None),
            P("dec", "ra", None, None),
            P(),
        ),
        out_specs=(P("dec", "ra"), P("dec", "ra")),
        check_vma=False,
    )
```

```python
import jax
import jax.numpy as jnp
from jax import lax
from jax.experimental import pallas as pl
from jax.experimental.pallas import tpu as pltpu
from jax.sharding import PartitionSpec as P


ROWS = 192
COLS = 256
PROWS = 320
PCOLS = 384
BAND = 96
EXT = 256
HALF = 31
SIDE = 63
LEFT = 64 - HALF
TILES_K = 33
PI = 3.141592653589793
F32 = jnp.float32
BF16 = jnp.bfloat16


def swap_pairs(block, axis, firsts, wrap):
    count = lax.axis_size(axis)
    lows = [i for i in range(count) if firsts(i) and (wrap or i + 1 < count)]
    if not lows:
        return jnp.zeros_like(block)
    pairs = [(i, (i + 1) % count) for i in lows]
    return lax.ppermute(block, axis, pairs + [(b, a) for a, b in pairs])


def gather_pairs(block, axis):
    count = lax.axis_size(axis)
    groups = [[i, i + 1] for i in range(0, count, 2)]
    return lax.all_gather(block, axis, axis_index_groups=groups)


def is_odd(axis):
    return (lax.axis_index(axis) & 1) == 1


def sin_pi(z):
    y = z * PI
    y2 = y * y
    poly = 1.0 / 6227020800.0
    for factorial in (-39916800.0, 362880.0, -5040.0, 120.0, -6.0, 1.0):
        poly = poly * y2 + 1.0 / factorial
    return y * poly


def lanczos_map(offset, fraction, direction):
    lane = lax.broadcasted_iota(jnp.int32, (8, 128), 1)
    signed = jnp.where(lane < 64, lane, lane - 128) * direction
    step = signed + offset
    where_at = step.astype(F32) + fraction
    parity = 1.0 - 2.0 * (step & 1).astype(F32)
    frac = jnp.full((8, 128), fraction, F32)
    third = jnp.abs(where_at) * (1.0 / 3.0)
    folded = jnp.where(third > 0.5, 1.0 - third, third)
    safe = jnp.where(where_at == 0.0, 1.0, where_at)
    first = parity * sin_pi(frac) / (safe * PI)
    second = sin_pi(folded) * 3.0 / (jnp.abs(safe) * PI)
    value = jnp.where(where_at == 0.0, 1.0, first * second)
    value = jnp.where(jnp.abs(where_at) < 3.0, value, 0.0)
    rows = jnp.broadcast_to(value[0:1], (128, 128))
    turned = pltpu.roll(rows, 0, 1, stride=1, stride_axis=0)
    down = lax.broadcasted_iota(jnp.int32, (128, 128), 0)
    across = lax.broadcasted_iota(jnp.int32, (128, 128), 1)
    gap = across - down
    diagonal = jnp.where(jnp.abs(gap) <= 64, turned, 0.0)
    upper = jnp.where(gap < -64, turned, 0.0)
    lower = jnp.where(gap > 64, turned, 0.0)
    return diagonal, upper, lower


def row_map(offset, fraction):
    return jnp.concatenate(split(lanczos_map(offset, fraction, -1)[0]), axis=1)


def col_map(offset, fraction):
    diagonal, upper, lower = lanczos_map(offset, fraction, 1)
    return split(
        jnp.concatenate(
            [
                jnp.concatenate([diagonal, upper], axis=1),
                jnp.concatenate([lower, diagonal], axis=1),
            ],
            axis=0,
        )
    )


def split(value):
    high = value.astype(BF16)
    return high, (value - high.astype(F32)).astype(BF16)


def dot(a, b):
    return lax.dot_general(a, b, (((1,), (0,)), ((), ())), preferred_element_type=F32)


def joined(left, right):
    lane = lax.broadcasted_iota(jnp.int32, left[:, :128].shape, 1)
    middle = jnp.where(lane < 64, left[:, 128:], right[:, :128])
    return jnp.concatenate([left[:, :128], middle, right[:, 128:]], axis=1)


def warp_cols(half, pair):
    return [
        [
            dot(half[:, at : at + 256], pair[0]) + dot(half[:, at : at + 256], pair[1])
            for at in (PCOLS * n, PCOLS * n + 128)
        ]
        for n in range(2)
    ]


def added(first, second):
    return [joined(*(a + b for a, b in zip(first[n], second[n]))) for n in range(2)]


def warp_kernel(
    off_hbm, sub_hbm, cov_hbm, exp_hbm, inv_hbm, val_hbm,
    own, near, far, middle, row_maps, col_maps,
    off, sub, cov, exp, inv, val, small, large,
):
    scalars = [
        pltpu.make_async_copy(source, target, small.at[i])
        for i, (source, target) in enumerate(((off_hbm, off), (sub_hbm, sub), (cov_hbm, cov)))
    ]
    pieces = ((0, 320),)
    images = [
        [
            [
                pltpu.make_async_copy(
                    source.at[e, pl.ds(at, size)], target.at[e, pl.ds(at, size)], large.at[e, p, i]
                )
                for i, (source, target) in enumerate(((inv_hbm, inv), (val_hbm, val), (exp_hbm, exp)))
            ]
            for p, (at, size) in enumerate(pieces)
        ]
        for e in range(2)
    ]
    order = [(0, 0), (1, 0)]
    for copy in scalars + [copy for e, p in order for copy in images[e][p]]:
        copy.start()

    def load(e, p):
        at, size = pieces[p]
        cut = pl.ds(at, size)
        for copy in images[e][p]:
            copy.wait()
        masked = inv[e, cut] * (val[e, cut].astype(F32) * cov[0, 0, e].astype(F32))
        return jnp.concatenate([masked * exp[e, cut], masked], axis=1).astype(BF16)

    for copy in scalars:
        copy.wait()
    rows = [row_map(off[0, 0, e, 0], sub[0, 0, e, 0]) for e in range(2)]
    cols = [col_map(off[0, 0, e, 1], sub[0, 0, e, 1]) for e in range(2)]
    sums = []
    for e in range(2):
        data = load(e, 0)
        middle[e] = data[80:256]
        parts = [
            dot(lhs, jnp.concatenate([data[at : at + 128]] * 2, axis=0))
            for lhs, at in ((rows[e][:96], 0), (rows[e][32:], 192))
        ]
        sums.append(warp_cols(jnp.concatenate(parts, axis=0).astype(BF16), cols[e]))
    for e in range(2):
        row_maps[e] = rows[e]
        col_maps[e, 0], col_maps[e, 1] = cols[e]
    odd = is_odd("dec")
    for n, whole in enumerate(added(*sums)):
        own[n, :64], own[n, 64:] = whole[32:96], whole[96:160]
        top, bottom = whole[:BAND], whole[BAND:]
        near[n] = jnp.where(odd, top, bottom).astype(BF16)
        far[n] = jnp.where(odd, bottom, top).astype(BF16)


def middle_kernel(middle, row_maps, col_maps, own):
    sums = []
    for e in range(2):
        parts = [
            dot(row_maps[e, low:high], jnp.concatenate([middle[e, at : at + 128]] * 2, axis=0))
            for low, high, at in ((16, 112, 0), (64, 96, 48))
        ]
        half = jnp.concatenate(parts, axis=0).astype(BF16)
        sums.append(warp_cols(half, (col_maps[e, 0], col_maps[e, 1])))
    own[0], own[1] = added(*sums)


def is_outer():
    strip = lax.axis_index("dec")
    return (strip == 0) | (strip == lax.axis_size("dec") - 1)


def dec_sum(own, mid, near, far, odd, n, block):
    cut = pl.ds(block * 128 if isinstance(block, int) else pl.multiple_of(block * 128, 128), 128)
    other = 1 - (lax.axis_index("dec") & 1)
    first, second = near[other, n, :, cut].astype(F32), far[n, :, cut].astype(F32)
    above, below = jnp.where(odd, first, second), jnp.where(odd, second, first)
    return jnp.concatenate(
        [
            own[n, :64, cut] + above[:64],
            mid[n, :32, cut] + above[64:],
            mid[n, 32:96, cut],
            mid[n, 96:, cut] + below[:32],
            own[n, 64:, cut] + below[32:],
        ],
        axis=0,
    )


def pack(planes):
    lane = lax.broadcasted_iota(jnp.int32, (128, 128), 1)
    groups = [plane[128 * i : 128 * i + 128] for plane in planes for i in range(2)]
    return jnp.concatenate(
        [
            jnp.where(lane < 96, groups[i], pltpu.roll(groups[3], 96 - 32 * i, 1))
            for i in range(3)
        ],
        axis=0,
    )


def unpack(packed):
    lane = lax.broadcasted_iota(jnp.int32, (128, 128), 1)
    groups = [packed[128 * i : 128 * i + 128] for i in range(3)]
    last = pltpu.roll(groups[0], 32, 1)
    last = jnp.where(lane < 32, last, pltpu.roll(groups[1], 64, 1))
    last = jnp.where(lane < 64, last, pltpu.roll(groups[2], 96, 1))
    groups.append(last)
    return [jnp.concatenate(groups[2 * n : 2 * n + 2], axis=0) for n in range(2)]


def edges_kernel(own, mid, near, far, one, two):
    odd = is_odd("dec")
    west = pack([dec_sum(own, mid, near, far, odd, n, 0) for n in range(2)])
    east = pack([pltpu.roll(dec_sum(own, mid, near, far, odd, n, 2), 96, 1) for n in range(2)])
    odd = is_odd("ra")
    one[...] = jnp.where(odd, west, east).astype(BF16)
    two[...] = jnp.where(odd, east, west).astype(BF16)


def psf_kernel(psf, weights, taps):
    down = lax.broadcasted_iota(jnp.int32, (SIDE, 128), 0)
    across = lax.broadcasted_iota(jnp.int32, (SIDE, 128), 1)
    reverse = jnp.where(((down + across) & 127) == 0, 1.0, 0.0).astype(BF16)
    taps[...] = jnp.zeros((80, 128), F32)
    taps[8 : 8 + SIDE] = dot(psf[...], reverse)
    lane = lax.broadcasted_iota(jnp.int32, (128, 128), 1)
    weights[0] = jnp.zeros((256, 128), BF16)
    weights[TILES_K] = jnp.zeros((256, 128), BF16)
    before = jnp.zeros((128, 128), F32)
    for q in range(64):
        here = jnp.broadcast_to(taps[8 + q : 9 + q], (128, 128))
        here = pltpu.roll(here, 0, 1, stride=1, stride_axis=0)
        prev = jnp.concatenate([before[64:], before[:64]], axis=0)
        weights[1 + q // 2, 128 * (q % 2) : 128 * (q % 2) + 128] = jnp.where(
            lane < 64, here, prev
        ).astype(BF16)
        before = here


def outer_fill_kernel(psf, middle, row_maps, col_maps, weights, own, taps):
    @pl.when(is_outer())
    def _():
        psf_kernel(psf, weights, taps)
        middle_kernel(middle, row_maps, col_maps, own)


def inner_fill_kernel(psf, middle, row_maps, col_maps, ready, ready_own, weights, own, taps):
    @pl.when(jnp.logical_not(is_outer()))
    def _():
        psf_kernel(psf, weights, taps)
        middle_kernel(middle, row_maps, col_maps, own)


def half_match(half, base, bands, weights, weight, windows, stage):
    lane = lax.broadcasted_iota(jnp.int32, (EXT, 128), 1)
    east = half == 1
    planes = []
    for n, band in enumerate(unpack(bands)):
        band = jnp.where(
            east, jnp.where(lane < 96, band, 0.0), jnp.where(lane >= 32, pltpu.roll(band, 32, 1), 0.0)
        )
        left, right = base(n)
        planes.append(
            jnp.concatenate(
                [left + jnp.where(east, 0.0, band), right + jnp.where(east, band, 0.0)], axis=1
            )
        )
    numer, denom = planes
    row = lax.broadcasted_iota(jnp.int32, (EXT, 256), 0) + (lax.axis_index("dec") * ROWS - 32)
    inside = (row >= 0) & (row < lax.axis_size("dec") * ROWS)
    coadd = jnp.where(inside, numer / jnp.maximum(denom, 1.0), 0.0).astype(BF16).astype(F32)
    weight(pltpu.roll(denom, 256 - 64, 1)[32 : 32 + ROWS, :128])
    for k in range(2):
        windows[k] = pltpu.roll(coadd, 256 - LEFT - 64 * k, 1)[:, :128]
    total = None
    for t in range(TILES_K):
        left = jnp.concatenate(
            [
                jnp.concatenate(
                    [windows[k, pl.ds(2 * t + s + 1, 48, stride=4), :] for k in range(2)], axis=0
                )
                for s in range(2)
            ],
            axis=1,
        ).astype(BF16)
        right = jnp.concatenate([weights[t + 1], weights[t]], axis=1)
        part = dot(left, right)
        total = part if total is None else total + part
    lane = lax.broadcasted_iota(jnp.int32, (48, 128), 1)
    for p in range(4):
        cut = slice(128 * (p // 2), 128 * (p // 2) + 128)
        low, high = total[:48, cut], total[48:, cut]
        if p % 2:
            low = pltpu.roll(low, 64, 1)
        else:
            high = pltpu.roll(high, 64, 1)
        stage[pl.ds(p, 48, stride=4), :] = jnp.where(lane < 64, low, high)


def first_kernel(own, mid, near, far, one, other, weights, out, weight_map, base, windows):
    def weight(value):
        weight_map[...] = value

    odd = is_odd("dec")

    def block(n, at):
        return dec_sum(own, mid, near, far, odd, n, at)

    half = 1 - (lax.axis_index("ra") & 1)
    for n in range(2):
        for i in range(2):
            base[n, i] = block(n, 1 - half + i)
    bands = one[...].astype(F32) + other[...].astype(F32)
    half_match(
        half, lambda n: (block(n, half), block(n, half + 1)), bands, weights, weight, windows, out
    )


def second_kernel(
    two, weights, ready, ready_weight, base,
    out, weight_map,
    windows, stage, stage_weight, sems,
):
    half = lax.axis_index("ra") & 1
    this, that = (pl.ds(pl.multiple_of(128 * x, 128), 128) for x in (half, 1 - half))
    copies = [
        pltpu.make_async_copy(source, target, sems.at[i])
        for i, (source, target) in enumerate(
            (
                (ready, out.at[:, that]),
                (ready_weight, weight_map.at[:, that]),
                (stage_weight, weight_map.at[:, this]),
                (stage, out.at[:, this]),
            )
        )
    ]
    copies[0].start()
    copies[1].start()

    def weight(value):
        stage_weight[...] = value
        copies[2].start()

    bands = two[...].astype(F32)
    half_match(
        half, lambda n: (base[n, 0], base[n, 1]), bands, weights, weight, windows, stage
    )
    copies[3].start()
    for copy in copies:
        copy.wait()


HBM = pl.BlockSpec(memory_space=pltpu.HBM)
VMEM = pl.BlockSpec(memory_space=pltpu.VMEM)


def call(body, ins, outs, scratch=(), flops=0, limit=16, space=None, aliases=None):
    return pl.pallas_call(
        body,
        in_specs=ins,
        out_specs=tuple(space or VMEM for _ in outs),
        out_shape=outs,
        scratch_shapes=scratch,
        input_output_aliases=aliases or {},
        cost_estimate=pl.CostEstimate(flops=flops, transcendentals=0, bytes_accessed=4_000_000),
        compiler_params=pltpu.CompilerParams(vmem_limit_bytes=limit * 1024 * 1024),
    )


def array(shape, kind):
    return jax.ShapeDtypeStruct(shape, kind)


def shards(exposures, inv_variance, pixel_valid, correlation, pixel_offset, subpixel, psf_match):
    own, near, far, middle, row_maps, col_maps = call(
        warp_kernel,
        [HBM] * 6,
        (
            array((2, 128, PCOLS), F32),
            array((2, BAND, PCOLS), BF16),
            array((2, BAND, PCOLS), BF16),
            array((2, 176, 2 * PCOLS), BF16),
            array((2, 128, 256), BF16),
            array((2, 2, 256, 256), BF16),
        ),
        scratch=[
            pltpu.SMEM((1, 1, 2, 2), jnp.int32),
            pltpu.SMEM((1, 1, 2, 2), F32),
            pltpu.SMEM((1, 1, 2), jnp.int32),
            pltpu.VMEM((2, PROWS, PCOLS), F32),
            pltpu.VMEM((2, PROWS, PCOLS), F32),
            pltpu.VMEM((2, PROWS, PCOLS), jnp.int32),
            pltpu.SemaphoreType.DMA((3,)),
            pltpu.SemaphoreType.DMA((2, 1, 3)),
        ],
        flops=3_000_000_000,
    )(
        *(
            pltpu.with_memory_space_constraint(x, pltpu.HBM)
            for x in (pixel_offset, subpixel, correlation, exposures, inv_variance, pixel_valid)
        )
    )
    filled = (array((TILES_K + 1, 256, 128), BF16), array((2, 128, PCOLS), F32))
    taps = [pltpu.VMEM((80, 128), F32)]
    far = swap_pairs(far, "dec", lambda i: i % 2 == 1, False)
    weights, mid = call(
        outer_fill_kernel, [VMEM] * 4, filled, taps, 3_000_000_000
    )(psf_match, middle, row_maps, col_maps)
    near = gather_pairs(near, "dec")
    weights, mid = call(
        inner_fill_kernel, [VMEM] * 6, filled, taps, 3_000_000_000, aliases={4: 0, 5: 1}
    )(psf_match, middle, row_maps, col_maps, weights, mid)
    one, two = call(
        edges_kernel,
        [VMEM] * 4,
        (array((384, 128), BF16), array((384, 128), BF16)),
        flops=1_000_000,
    )(own, mid, near, far)
    first = swap_pairs(one, "ra", lambda i: i % 8 in (0, 2, 4), True)
    two = swap_pairs(two, "ra", lambda i: i % 2 == 1, True)
    last = swap_pairs(one, "ra", lambda i: i % 8 == 6, True)
    windows = pltpu.VMEM((2, EXT, 128), F32)
    stage = pltpu.VMEM((ROWS, 128), F32)
    ready, ready_weight, base = call(
        first_kernel,
        [VMEM] * 7,
        (
            array((ROWS, 128), F32),
            array((ROWS, 128), F32),
            array((2, 2, EXT, 128), F32),
        ),
        scratch=[windows],
        flops=3_000_000_000,
    )(own, mid, near, far, first, last, weights)
    return call(
        second_kernel,
        [VMEM] * 5,
        (array((ROWS, COLS), F32), array((ROWS, COLS), F32)),
        scratch=[windows, stage, stage, pltpu.SemaphoreType.DMA((4,))],
        flops=3_000_000_000,
        space=HBM,
    )(two, weights, ready, ready_weight, base)


def solution(mesh):
    return jax.shard_map(
        shards,
        mesh=mesh,
        in_specs=(
            P(None, "dec", "ra"),
            P(None, "dec", "ra"),
            P(None, "dec", "ra"),
            P("dec", "ra", None),
            P("dec", "ra", None, None),
            P("dec", "ra", None, None),
            P(),
        ),
        out_specs=(P("dec", "ra"), P("dec", "ra")),
        check_vma=False,
    )
```

```python
import jax
import jax.numpy as jnp
from jax import lax
from jax.experimental import pallas as pl
from jax.experimental.pallas import tpu as pltpu
from jax.sharding import PartitionSpec as P


ROWS = 192
COLS = 256
PROWS = 320
PCOLS = 384
BAND = 96
EXT = 256
HALF = 31
SIDE = 63
LEFT = 64 - HALF
TILES_K = 33
PI = 3.141592653589793
F32 = jnp.float32
BF16 = jnp.bfloat16


def swap_pairs(block, axis, firsts, wrap):
    count = lax.axis_size(axis)
    lows = [i for i in range(count) if firsts(i) and (wrap or i + 1 < count)]
    if not lows:
        return jnp.zeros_like(block)
    pairs = [(i, (i + 1) % count) for i in lows]
    return lax.ppermute(block, axis, pairs + [(b, a) for a, b in pairs])


def gather_pairs(block, axis):
    count = lax.axis_size(axis)
    groups = [[i, i + 1] for i in range(0, count, 2)]
    return lax.all_gather(block, axis, axis_index_groups=groups)


def is_odd(axis):
    return (lax.axis_index(axis) & 1) == 1


def sin_pi(z):
    y = z * PI
    y2 = y * y
    poly = 1.0 / 6227020800.0
    for factorial in (-39916800.0, 362880.0, -5040.0, 120.0, -6.0, 1.0):
        poly = poly * y2 + 1.0 / factorial
    return y * poly


def lanczos_map(offset, fraction, direction):
    lane = lax.broadcasted_iota(jnp.int32, (8, 128), 1)
    signed = jnp.where(lane < 64, lane, lane - 128) * direction
    step = signed + offset
    where_at = step.astype(F32) + fraction
    parity = 1.0 - 2.0 * (step & 1).astype(F32)
    frac = jnp.full((8, 128), fraction, F32)
    third = jnp.abs(where_at) * (1.0 / 3.0)
    folded = jnp.where(third > 0.5, 1.0 - third, third)
    safe = jnp.where(where_at == 0.0, 1.0, where_at)
    first = parity * sin_pi(frac) / (safe * PI)
    second = sin_pi(folded) * 3.0 / (jnp.abs(safe) * PI)
    value = jnp.where(where_at == 0.0, 1.0, first * second)
    value = jnp.where(jnp.abs(where_at) < 3.0, value, 0.0)
    rows = jnp.broadcast_to(value[0:1], (128, 128))
    turned = pltpu.roll(rows, 0, 1, stride=1, stride_axis=0)
    down = lax.broadcasted_iota(jnp.int32, (128, 128), 0)
    across = lax.broadcasted_iota(jnp.int32, (128, 128), 1)
    gap = across - down
    diagonal = jnp.where(jnp.abs(gap) <= 64, turned, 0.0)
    upper = jnp.where(gap < -64, turned, 0.0)
    lower = jnp.where(gap > 64, turned, 0.0)
    return diagonal, upper, lower


def row_map(offset, fraction):
    return jnp.concatenate(split(lanczos_map(offset, fraction, -1)[0]), axis=1)


def col_map(offset, fraction):
    diagonal, upper, lower = lanczos_map(offset, fraction, 1)
    return split(
        jnp.concatenate(
            [
                jnp.concatenate([diagonal, upper], axis=1),
                jnp.concatenate([lower, diagonal], axis=1),
            ],
            axis=0,
        )
    )


def split(value):
    high = value.astype(BF16)
    return high, (value - high.astype(F32)).astype(BF16)


def dot(a, b):
    return lax.dot_general(a, b, (((1,), (0,)), ((), ())), preferred_element_type=F32)


def joined(left, right):
    lane = lax.broadcasted_iota(jnp.int32, left[:, :128].shape, 1)
    middle = jnp.where(lane < 64, left[:, 128:], right[:, :128])
    return jnp.concatenate([left[:, :128], middle, right[:, 128:]], axis=1)


def warp_cols(half, pair):
    return [
        [
            dot(half[:, at : at + 256], pair[0]) + dot(half[:, at : at + 256], pair[1])
            for at in (PCOLS * n, PCOLS * n + 128)
        ]
        for n in range(2)
    ]


def added(first, second):
    return [joined(*(a + b for a, b in zip(first[n], second[n]))) for n in range(2)]


def warp_kernel(
    off_hbm, sub_hbm, cov_hbm, exp_hbm, inv_hbm, val_hbm,
    own, near, far, middle, row_maps, col_maps,
    off, sub, cov, exp, inv, val, small, large,
):
    scalars = [
        pltpu.make_async_copy(source, target, small.at[i])
        for i, (source, target) in enumerate(((off_hbm, off), (sub_hbm, sub), (cov_hbm, cov)))
    ]
    pieces = ((0, 320),)
    images = [
        [
            [
                pltpu.make_async_copy(
                    source.at[e, pl.ds(at, size)], target.at[e, pl.ds(at, size)], large.at[e, p, i]
                )
                for i, (source, target) in enumerate(((inv_hbm, inv), (val_hbm, val), (exp_hbm, exp)))
            ]
            for p, (at, size) in enumerate(pieces)
        ]
        for e in range(2)
    ]
    order = [(0, 0), (1, 0)]
    for copy in scalars + [copy for e, p in order for copy in images[e][p]]:
        copy.start()

    def load(e, p):
        at, size = pieces[p]
        cut = pl.ds(at, size)
        for copy in images[e][p]:
            copy.wait()
        masked = inv[e, cut] * (val[e, cut].astype(F32) * cov[0, 0, e].astype(F32))
        return jnp.concatenate([masked * exp[e, cut], masked], axis=1).astype(BF16)

    for copy in scalars:
        copy.wait()
    rows = [row_map(off[0, 0, e, 0], sub[0, 0, e, 0]) for e in range(2)]
    cols = [col_map(off[0, 0, e, 1], sub[0, 0, e, 1]) for e in range(2)]
    sums = []
    for e in range(2):
        data = load(e, 0)
        middle[e] = data[80:256]
        parts = [
            dot(lhs, jnp.concatenate([data[at : at + 128]] * 2, axis=0))
            for lhs, at in ((rows[e][:96], 0), (rows[e][32:], 192))
        ]
        sums.append(warp_cols(jnp.concatenate(parts, axis=0).astype(BF16), cols[e]))
    for e in range(2):
        row_maps[e] = rows[e]
        col_maps[e, 0], col_maps[e, 1] = cols[e]
    odd = is_odd("dec")
    for n, whole in enumerate(added(*sums)):
        own[n, :64], own[n, 64:] = whole[32:96], whole[96:160]
        top, bottom = whole[:BAND], whole[BAND:]
        near[n] = jnp.where(odd, top, bottom).astype(BF16)
        far[n] = jnp.where(odd, bottom, top).astype(BF16)


def middle_kernel(middle, row_maps, col_maps, own):
    sums = []
    for e in range(2):
        parts = [
            dot(row_maps[e, low:high], jnp.concatenate([middle[e, at : at + 128]] * 2, axis=0))
            for low, high, at in ((16, 112, 0), (64, 96, 48))
        ]
        half = jnp.concatenate(parts, axis=0).astype(BF16)
        sums.append(warp_cols(half, (col_maps[e, 0], col_maps[e, 1])))
    own[0], own[1] = added(*sums)


def is_outer():
    strip = lax.axis_index("dec")
    return (strip == 0) | (strip == lax.axis_size("dec") - 1)


def dec_sum(own, mid, near, far, odd, n, block):
    cut = pl.ds(block * 128 if isinstance(block, int) else pl.multiple_of(block * 128, 128), 128)
    other = 1 - (lax.axis_index("dec") & 1)
    first, second = near[other, n, :, cut].astype(F32), far[n, :, cut].astype(F32)
    above, below = jnp.where(odd, first, second), jnp.where(odd, second, first)
    return jnp.concatenate(
        [
            own[n, :64, cut] + above[:64],
            mid[n, :32, cut] + above[64:],
            mid[n, 32:96, cut],
            mid[n, 96:, cut] + below[:32],
            own[n, 64:, cut] + below[32:],
        ],
        axis=0,
    )


def pack(planes):
    lane = lax.broadcasted_iota(jnp.int32, (128, 128), 1)
    groups = [plane[128 * i : 128 * i + 128] for plane in planes for i in range(2)]
    return jnp.concatenate(
        [
            jnp.where(lane < 96, groups[i], pltpu.roll(groups[3], 96 - 32 * i, 1))
            for i in range(3)
        ],
        axis=0,
    )


def unpack(packed):
    lane = lax.broadcasted_iota(jnp.int32, (128, 128), 1)
    groups = [packed[128 * i : 128 * i + 128] for i in range(3)]
    last = pltpu.roll(groups[0], 32, 1)
    last = jnp.where(lane < 32, last, pltpu.roll(groups[1], 64, 1))
    last = jnp.where(lane < 64, last, pltpu.roll(groups[2], 96, 1))
    groups.append(last)
    return [jnp.concatenate(groups[2 * n : 2 * n + 2], axis=0) for n in range(2)]


def edges_kernel(own, mid, near, far, one, two):
    odd = is_odd("dec")
    west = pack([dec_sum(own, mid, near, far, odd, n, 0) for n in range(2)])
    east = pack([pltpu.roll(dec_sum(own, mid, near, far, odd, n, 2), 96, 1) for n in range(2)])
    odd = is_odd("ra")
    one[...] = jnp.where(odd, west, east).astype(BF16)
    two[...] = jnp.where(odd, east, west).astype(BF16)


def psf_kernel(psf, weights, taps):
    down = lax.broadcasted_iota(jnp.int32, (SIDE, 128), 0)
    across = lax.broadcasted_iota(jnp.int32, (SIDE, 128), 1)
    reverse = jnp.where(((down + across) & 127) == 0, 1.0, 0.0).astype(BF16)
    taps[...] = jnp.zeros((80, 128), F32)
    taps[8 : 8 + SIDE] = dot(psf[...], reverse)
    lane = lax.broadcasted_iota(jnp.int32, (128, 128), 1)
    weights[0] = jnp.zeros((256, 128), BF16)
    weights[TILES_K] = jnp.zeros((256, 128), BF16)
    before = jnp.zeros((128, 128), F32)
    for q in range(64):
        here = jnp.broadcast_to(taps[8 + q : 9 + q], (128, 128))
        here = pltpu.roll(here, 0, 1, stride=1, stride_axis=0)
        prev = jnp.concatenate([before[64:], before[:64]], axis=0)
        weights[1 + q // 2, 128 * (q % 2) : 128 * (q % 2) + 128] = jnp.where(
            lane < 64, here, prev
        ).astype(BF16)
        before = here


def outer_fill_kernel(psf, middle, row_maps, col_maps, weights, own, taps):
    @pl.when(is_outer())
    def _():
        psf_kernel(psf, weights, taps)
        middle_kernel(middle, row_maps, col_maps, own)


def inner_fill_kernel(psf, middle, row_maps, col_maps, ready, ready_own, weights, own, taps):
    @pl.when(jnp.logical_not(is_outer()))
    def _():
        psf_kernel(psf, weights, taps)
        middle_kernel(middle, row_maps, col_maps, own)


def half_match(half, base, bands, weights, weight, windows, stage):
    east = half == 1
    planes = []
    for n, band in enumerate(unpack(bands)):
        band = pltpu.roll(band, 32 * (1 - half), 1)
        left, right = base(n)
        planes.append(
            jnp.concatenate(
                [left + jnp.where(east, 0.0, band), right + jnp.where(east, band, 0.0)], axis=1
            )
        )
    numer, denom = planes
    row = lax.broadcasted_iota(jnp.int32, (EXT, 256), 0) + (lax.axis_index("dec") * ROWS - 32)
    inside = (row >= 0) & (row < lax.axis_size("dec") * ROWS)
    coadd = jnp.where(inside, numer / jnp.maximum(denom, 1.0), 0.0).astype(BF16).astype(F32)
    weight(pltpu.roll(denom, 256 - 64, 1)[32 : 32 + ROWS, :128])
    for k in range(2):
        windows[k] = pltpu.roll(coadd, 256 - LEFT - 64 * k, 1)[:, :128]
    total = None
    for t in range(TILES_K):
        left = jnp.concatenate(
            [
                jnp.concatenate(
                    [windows[k, pl.ds(2 * t + s + 1, 48, stride=4), :] for k in range(2)], axis=0
                )
                for s in range(2)
            ],
            axis=1,
        ).astype(BF16)
        right = jnp.concatenate([weights[t + 1], weights[t]], axis=1)
        part = dot(left, right)
        total = part if total is None else total + part
    lane = lax.broadcasted_iota(jnp.int32, (48, 128), 1)
    for p in range(4):
        cut = slice(128 * (p // 2), 128 * (p // 2) + 128)
        low, high = total[:48, cut], total[48:, cut]
        if p % 2:
            low = pltpu.roll(low, 64, 1)
        else:
            high = pltpu.roll(high, 64, 1)
        stage[pl.ds(p, 48, stride=4), :] = jnp.where(lane < 64, low, high)


def first_kernel(own, mid, near, far, one, other, weights, out, weight_map, base, windows):
    def weight(value):
        weight_map[...] = value

    odd = is_odd("dec")

    def block(n, at):
        return dec_sum(own, mid, near, far, odd, n, at)

    half = 1 - (lax.axis_index("ra") & 1)
    for n in range(2):
        for i in range(2):
            base[n, i] = block(n, 1 - half + i)
    bands = one[...].astype(F32) + other[...].astype(F32)
    half_match(
        half, lambda n: (block(n, half), block(n, half + 1)), bands, weights, weight, windows, out
    )


def second_kernel(
    two, weights, ready, ready_weight, base,
    out, weight_map,
    windows, stage, stage_weight, sems,
):
    half = lax.axis_index("ra") & 1
    this, that = (pl.ds(pl.multiple_of(128 * x, 128), 128) for x in (half, 1 - half))
    copies = [
        pltpu.make_async_copy(source, target, sems.at[i])
        for i, (source, target) in enumerate(
            (
                (ready, out.at[:, that]),
                (ready_weight, weight_map.at[:, that]),
                (stage_weight, weight_map.at[:, this]),
                (stage, out.at[:, this]),
            )
        )
    ]
    copies[0].start()
    copies[1].start()

    def weight(value):
        stage_weight[...] = value
        copies[2].start()

    bands = two[...].astype(F32)
    half_match(
        half, lambda n: (base[n, 0], base[n, 1]), bands, weights, weight, windows, stage
    )
    copies[3].start()
    for copy in copies:
        copy.wait()


HBM = pl.BlockSpec(memory_space=pltpu.HBM)
VMEM = pl.BlockSpec(memory_space=pltpu.VMEM)


def call(body, ins, outs, scratch=(), flops=0, limit=16, space=None, aliases=None):
    return pl.pallas_call(
        body,
        in_specs=ins,
        out_specs=tuple(space or VMEM for _ in outs),
        out_shape=outs,
        scratch_shapes=scratch,
        input_output_aliases=aliases or {},
        cost_estimate=pl.CostEstimate(flops=flops, transcendentals=0, bytes_accessed=4_000_000),
        compiler_params=pltpu.CompilerParams(vmem_limit_bytes=limit * 1024 * 1024),
    )


def array(shape, kind):
    return jax.ShapeDtypeStruct(shape, kind)


def shards(exposures, inv_variance, pixel_valid, correlation, pixel_offset, subpixel, psf_match):
    own, near, far, middle, row_maps, col_maps = call(
        warp_kernel,
        [HBM] * 6,
        (
            array((2, 128, PCOLS), F32),
            array((2, BAND, PCOLS), BF16),
            array((2, BAND, PCOLS), BF16),
            array((2, 176, 2 * PCOLS), BF16),
            array((2, 128, 256), BF16),
            array((2, 2, 256, 256), BF16),
        ),
        scratch=[
            pltpu.SMEM((1, 1, 2, 2), jnp.int32),
            pltpu.SMEM((1, 1, 2, 2), F32),
            pltpu.SMEM((1, 1, 2), jnp.int32),
            pltpu.VMEM((2, PROWS, PCOLS), F32),
            pltpu.VMEM((2, PROWS, PCOLS), F32),
            pltpu.VMEM((2, PROWS, PCOLS), jnp.int32),
            pltpu.SemaphoreType.DMA((3,)),
            pltpu.SemaphoreType.DMA((2, 1, 3)),
        ],
        flops=3_000_000_000,
    )(
        *(
            pltpu.with_memory_space_constraint(x, pltpu.HBM)
            for x in (pixel_offset, subpixel, correlation, exposures, inv_variance, pixel_valid)
        )
    )
    filled = (array((TILES_K + 1, 256, 128), BF16), array((2, 128, PCOLS), F32))
    taps = [pltpu.VMEM((80, 128), F32)]
    far = swap_pairs(far, "dec", lambda i: i % 2 == 1, False)
    weights, mid = call(
        outer_fill_kernel, [VMEM] * 4, filled, taps, 3_000_000_000
    )(psf_match, middle, row_maps, col_maps)
    near = gather_pairs(near, "dec")
    weights, mid = call(
        inner_fill_kernel, [VMEM] * 6, filled, taps, 3_000_000_000, aliases={4: 0, 5: 1}
    )(psf_match, middle, row_maps, col_maps, weights, mid)
    one, two = call(
        edges_kernel,
        [VMEM] * 4,
        (array((384, 128), BF16), array((384, 128), BF16)),
        flops=1_000_000,
    )(own, mid, near, far)
    first = swap_pairs(one, "ra", lambda i: i % 8 in (0, 2, 4), True)
    two = swap_pairs(two, "ra", lambda i: i % 2 == 1, True)
    last = swap_pairs(one, "ra", lambda i: i % 8 == 6, True)
    windows = pltpu.VMEM((2, EXT, 128), F32)
    stage = pltpu.VMEM((ROWS, 128), F32)
    ready, ready_weight, base = call(
        first_kernel,
        [VMEM] * 7,
        (
            array((ROWS, 128), F32),
            array((ROWS, 128), F32),
            array((2, 2, EXT, 128), F32),
        ),
        scratch=[windows],
        flops=3_000_000_000,
    )(own, mid, near, far, first, last, weights)
    return call(
        second_kernel,
        [VMEM] * 5,
        (array((ROWS, COLS), F32), array((ROWS, COLS), F32)),
        scratch=[windows, stage, stage, pltpu.SemaphoreType.DMA((4,))],
        flops=3_000_000_000,
        space=HBM,
    )(two, weights, ready, ready_weight, base)


def solution(mesh):
    return jax.shard_map(
        shards,
        mesh=mesh,
        in_specs=(
            P(None, "dec", "ra"),
            P(None, "dec", "ra"),
            P(None, "dec", "ra"),
            P("dec", "ra", None),
            P("dec", "ra", None, None),
            P("dec", "ra", None, None),
            P(),
        ),
        out_specs=(P("dec", "ra"), P("dec", "ra")),
        check_vma=False,
    )
```
